32 devices in a mesh: gx: 4 (over z), gy: 8 (over y, x, core).
Axes of the slice: x: 2, y: 2, z: 4, core: 2. Of those that a mesh axis runs over, the one named last changes fastest.
Arguments:
- gradient: float32 [32, 2048], P('gx', 'gy'), may hold values from -6 to 6
- warm_start: float32 [32, 2048], P('gx', 'gy'), may hold values from -3 to 3
- viscosity: float32 [32, 32, 2048], P(None, 'gx', 'gy'), may hold values from 1 to 10
- friction_coef: float32 [32, 2048], P('gx', 'gy'), may hold values from 0.5 to 5
- slide_dir: float32 [2, 32, 2048], P(None, 'gx', 'gy'), may hold values from -4 to 4
- obs_weight: float32 [32, 2048], P('gx', 'gy'), may hold values from 0.5 to 2
- ice_mask: int32 [32, 2048], P('gx', 'gy'), may hold values 0 or 1
- grounded: int32 [32, 2048], P('gx', 'gy'), may hold values 0 or 1
Outputs:
- solution: float32 [32, 2048], P('gx', 'gy')
- residual: float32 [32, 2048], P('gx', 'gy')
The draws below stay inside these ranges and needn't reach their ends.
All inputs are finite; a program needn't handle non-finite values. No bound on the sum of `ice_mask` or of `grounded` on one device may be relied on, other than what follows from the above.
Results may differ from the reference program's by a relative error of at most 0.00075.
Values sent between devices are 32-bit elements; how exact they have to be, the bound alone decides.
No kernel may reach another device: no remote copies, remote signals or barrier semaphores. Data moves between devices by JAX's collectives and lax.ppermute only.
A program may use at most 128 MiB of HBM per device.

```python
import math
import jax
import jax.numpy as jnp

NZ = 32
ITERS = 2
NX = 32
NY = 2048


def plant(entries, rng, smallest, high):
    spot = [jax.random.randint(jax.random.fold_in(rng, axis), (), 0, length) for axis, length in enumerate(entries.shape)]
    longest = entries.shape.index(max(entries.shape))
    neighbour = spot[:longest] + [(spot[longest] + 1) % entries.shape[longest]] + spot[longest + 1:]
    return entries.at[tuple(spot)].set(smallest).at[tuple(neighbour)].set(high)


def block_levels(own_key, dims, shards, smallest, high):
    def one(dim, parts):
        steps = jax.random.uniform(jax.random.fold_in(jax.random.fold_in(own_key, 6), dim), (parts,), jnp.float32, smallest / len(shards), high / len(shards))
        return jnp.repeat(jnp.exp(steps), dims[dim] // parts).reshape((-1,) + (1,) * (len(dims) - dim - 1))

    gain = one(*shards[0])
    for cut in shards[1:]:
        gain = gain * one(*cut)
    return gain


def normal_values(key, dims, scale, limit, pieces=(), kind=jnp.bfloat16):
    values = jax.random.normal(key, dims, jnp.float32) * scale
    if len(pieces) > 0:
        values = block_levels(key, dims, pieces, -0.22, 0.18) * values
    return jnp.clip(values, min=-limit, max=limit).astype(kind)


def setup_inputs(seed: int = 0) -> dict:
    keys = jax.random.split(jax.random.key(seed), 9)
    gradient = normal_values(keys[0], (NX, NY), 1.0, 6.0, ((0, 4), (1, 8)), jnp.float32)
    warm_start = normal_values(keys[1], (NX, NY), 0.5, 3.0, ((0, 4), (1, 8)), jnp.float32)
    viscosity = jnp.clip(jnp.exp(math.log(10.0) - 2.3025851 * jax.random.uniform(keys[2], (NZ, NX, NY), jnp.float32) ** block_levels(keys[2], (NZ, NX, NY), ((1, 4), (2, 8)), -0.2, 0.2)), 1.0, 10.0)
    friction_coef = jnp.clip(jnp.exp(math.log(5.0) - 2.3025851 * jax.random.uniform(keys[3], (NX, NY), jnp.float32) ** block_levels(keys[3], (NX, NY), ((0, 4), (1, 8)), -0.2, 0.2)), 0.5, 5.0)
    slide_dir = normal_values(keys[4], (2, NX, NY), 1.0, 4.0, ((1, 4), (2, 8)), jnp.float32)
    obs_weight = jnp.clip(jnp.exp(math.log(2.0) - 1.3862944 * jax.random.uniform(keys[5], (NX, NY), jnp.float32) ** block_levels(keys[5], (NX, NY), ((0, 4), (1, 8)), -0.2, 0.2)), 0.5, 2.0)
    ice_mask = plant((jax.random.randint(keys[6], (NX, NY), 0, 8) < 7).astype(jnp.int32), jax.random.fold_in(keys[6], 1), 0, 1)
    grounded = plant((jax.random.randint(keys[7], (NX, NY), 0, 4) < 3).astype(jnp.int32), jax.random.fold_in(keys[7], 1), 0, 1)
    return {"gradient": gradient, "warm_start": warm_start, "viscosity": viscosity, "friction_coef": friction_coef, "slide_dir": slide_dir, "obs_weight": obs_weight, "ice_mask": ice_mask, "grounded": grounded}


vert_coupling = 128.0
sink_rate = 0.0625
bed_drag = 0.5
offset_weight = 0.0019
cross_share = 0.5
reg_gamma = 0.02
reg_smooth = 1.0
diag_scale = 0.003

neighbour_offsets = [(step_z, step_x, step_y) for step_z in (-1, 0, 1) for step_x in (-1, 0, 1) for step_y in (-1, 0, 1) if step_x != 0 or step_y != 0]


def couple(field_ext, eta_ext):
    levels = eta_ext.shape[0]
    span_x = eta_ext.shape[1] - 2
    span_y = eta_ext.shape[2] - 2
    padded_field = jnp.pad(field_ext, ((0, 0), (1, 1), (0, 0), (0, 0)))
    padded_eta = jnp.pad(eta_ext, ((1, 1), (0, 0), (0, 0)))
    center = eta_ext[:, 1:1 + span_x, 1:1 + span_y]
    along_one = jnp.zeros((levels, span_x, span_y), jnp.float32)
    along_two = jnp.zeros((levels, span_x, span_y), jnp.float32)
    for step_z, step_x, step_y in neighbour_offsets:
        near_eta = padded_eta[1 + step_z:1 + step_z + levels, 1 + step_x:1 + step_x + span_x, 1 + step_y:1 + step_y + span_y]
        weight = (offset_weight / (abs(step_x) + abs(step_y) + abs(step_z))) * 0.5 * (center + near_eta)
        near_field = padded_field[:, 1 + step_z:1 + step_z + levels, 1 + step_x:1 + step_x + span_x, 1 + step_y:1 + step_y + span_y]
        along_one = along_one + weight * near_field[0]
        along_two = along_two + weight * near_field[1]
        if step_x != 0 and step_y != 0:
            twist_weight = (cross_share * step_x * step_y) * weight
            along_one = along_one + twist_weight * near_field[1]
            along_two = along_two + twist_weight * near_field[0]
    return jnp.stack([along_one, along_two])


def tridiagonal(link_weights, diagonal, rhs_cols):
    levels = diagonal.shape[0]
    pivot_value = diagonal[0]
    ratios = [-link_weights[0] / pivot_value]
    partial_value = [rhs_cols[:, 0] / pivot_value]
    for layer_index in range(1, levels):
        pivot_value = diagonal[layer_index] + link_weights[layer_index - 1] * ratios[-1]
        partial_value.append((rhs_cols[:, layer_index] + link_weights[layer_index - 1] * partial_value[-1]) / pivot_value)
        if layer_index < levels - 1:
            ratios.append(-link_weights[layer_index] / pivot_value)
    result = [partial_value[-1]]
    for layer_index in range(levels - 2, -1, -1):
        result.insert(0, partial_value[layer_index] - ratios[layer_index] * result[0])
    return jnp.stack(result, axis=1)


def responses(viscosity, friction):
    levels = viscosity.shape[0]
    link_weights = vert_coupling * 0.5 * (viscosity[:-1] + viscosity[1:])
    zero_layer = jnp.zeros_like(viscosity[:1])
    diagonal = jnp.concatenate([zero_layer, link_weights]) + jnp.concatenate([link_weights, zero_layer]) + sink_rate * viscosity
    diagonal = diagonal.at[0].add(bed_drag * friction)
    unit_rhs = jnp.zeros((2,) + viscosity.shape, jnp.float32)
    unit_rhs = unit_rhs.at[0, 0].set(1.0).at[1, levels - 1].set(1.0)
    solved = tridiagonal(link_weights, diagonal, unit_rhs)
    return solved[0], solved[1]


def regularize(centre_ext):
    middle = centre_ext[1:-1, 1:-1]
    beside_all = centre_ext[2:, 1:-1] + centre_ext[:-2, 1:-1] + centre_ext[1:-1, 2:] + centre_ext[1:-1, :-2]
    return reg_gamma * (middle + reg_smooth * (4.0 * middle - beside_all))


def reference(gradient, warm_start, viscosity, friction_coef, slide_dir, obs_weight, ice_mask, grounded):
    ice_float = ice_mask.astype(jnp.float32)
    ground_float = grounded.astype(jnp.float32)
    friction = ground_float * friction_coef
    source = (ice_float * ground_float * friction_coef)[None] * slide_dir
    obs = ice_float * obs_weight
    inverse_diag = 1.0 / (reg_gamma * (1.0 + 4.0 * reg_smooth) + diag_scale * ice_float * ground_float * friction_coef * friction_coef)
    bottom_resp, top_resp = responses(viscosity, friction)
    eta_ext = jnp.pad(viscosity, ((0, 0), (1, 1), (1, 1)))

    def hessian(direction):
        spread = source * direction[None]
        first_state = bottom_resp[None] * spread[:, None]
        coupled = couple(jnp.pad(first_state, ((0, 0), (0, 0), (1, 1), (1, 1))), eta_ext)
        surface = spread * bottom_resp[-1][None] + jnp.sum(top_resp[None] * coupled, axis=1)
        traction = obs[None] * surface
        second_state = top_resp[None] * traction[:, None]
        coupled_back = couple(jnp.pad(second_state, ((0, 0), (0, 0), (1, 1), (1, 1))), eta_ext)
        basal_part = traction * top_resp[0][None] + jnp.sum(bottom_resp[None] * coupled_back, axis=1)
        return jnp.sum(source * basal_part, axis=0) + regularize(jnp.pad(direction, 1))

    solution = warm_start
    residual = gradient - hessian(warm_start)
    precond = inverse_diag * residual
    direction = precond
    norm_now = jnp.sum(residual * precond)
    for iteration in range(ITERS):
        image_vec = hessian(direction)
        step_size = norm_now / jnp.sum(direction * image_vec)
        solution = solution + step_size * direction
        residual = residual - step_size * image_vec
        precond = inverse_diag * residual
        norm_next = jnp.sum(residual * precond)
        direction = precond + (norm_next / norm_now) * direction
        norm_now = norm_next
    return solution, residual
```

```python
import jax
import jax.numpy as jnp
from jax import lax
from jax.experimental import pallas as pl
from jax.experimental.pallas import tpu as pltpu
from jax.sharding import PartitionSpec as P

vert_coupling = 128.0
sink_rate = 0.0625
bed_drag = 0.5
offset_weight = 0.0019
cross_share = 0.5
reg_gamma = 0.02
reg_smooth = 1.0
diag_scale = 0.003

HALO = 6
FIELDS = 7


def round_up(value, step):
    return -(-value // step) * step


def moved(block, step_x, step_y):
    if step_y:
        block = pltpu.roll(block, (-step_y) % block.shape[1], 1)
    if step_x:
        block = pltpu.roll(block, (-step_x) % block.shape[0], 0)
    return block


def vertical(visc_ref, friction, outside, up_ref, down_ref):
    levels = visc_ref.shape[0] - FIELDS
    half = 0.5 * vert_coupling
    inside = 1.0 - outside

    def eliminate(k, carry):
        low, high = carry
        up_here = visc_ref[k] + outside
        up_next = visc_ref[k + 1] + outside
        link = half * (up_here + up_next)
        ratio = link / (link + low)
        up_ref[k] = ratio
        low = sink_rate * up_next + ratio * low
        m = levels - 2 - k
        down_here = visc_ref[m + 1] + outside
        down_next = visc_ref[m] + outside
        link = half * (down_here + down_next)
        ratio = link / (link + high)
        down_ref[m + 1] = ratio
        high = sink_rate * down_next + ratio * high
        return low, high

    low = sink_rate * (visc_ref[0] + outside) + bed_drag * friction
    high = sink_rate * (visc_ref[levels - 1] + outside)
    low, high = lax.fori_loop(0, levels - 1, eliminate, (low, high))
    top = inside / low
    bed = inside / (high + bed_drag * friction)
    up_ref[levels - 1] = top
    down_ref[0] = bed

    def substitute(k, carry):
        top, bed = carry
        m = levels - 2 - k
        top = up_ref[m] * top
        up_ref[m] = top
        bed = down_ref[k + 1] * bed
        down_ref[k + 1] = bed
        return top, bed

    top, bed = lax.fori_loop(0, levels - 1, substitute, (top, bed))
    return top


def couplings(visc_ref, up_ref, down_ref):
    levels = visc_ref.shape[0] - FIELDS
    shape = visc_ref.shape[1:]
    result = {}
    for step_x in (-1, 0, 1):
        steps_y = (-1, 1) if step_x == 0 else (-1, 0, 1)

        def layer(k, carry, step_x=step_x, steps_y=steps_y):
            sums = carry
            below = jnp.maximum(k - 1, 0)
            above = jnp.minimum(k + 1, levels - 1)
            has_below = jnp.where(k > 0, 1.0, 0.0)
            has_above = jnp.where(k < levels - 1, 1.0, 0.0)
            here = down_ref[k]
            lower = down_ref[below] * has_below
            upper = down_ref[above] * has_above
            sides = lower + upper
            v_here = here * visc_ref[k]
            v_sides = lower * visc_ref[below] + upper * visc_ref[above]
            reach = {}
            for count in (1, 2):
                near = offset_weight * 0.5 / count
                far = offset_weight * 0.5 / (count + 1)
                reach[count] = (near * here + far * sides, near * v_here + far * v_sides)
            top = up_ref[k]
            v_top = moved(top * visc_ref[k], step_x, 0)
            top = moved(top, step_x, 0)
            out = []
            for total, step_y in zip(sums, steps_y):
                plain, heavy = reach[abs(step_x) + abs(step_y)]
                out.append(
                    total + moved(v_top, 0, step_y) * plain + moved(top, 0, step_y) * heavy
                )
            return tuple(out)

        zero = jnp.zeros(shape, jnp.float32)
        sums = lax.fori_loop(0, levels, layer, (zero,) * len(steps_y))
        for step_y, total in zip(steps_y, sums):
            result[step_x, step_y] = total
    return result


def spread(weights, centre, one, two):
    plus = (one + cross_share * two, two + cross_share * one)
    minus = (one - cross_share * two, two - cross_share * one)
    out = [centre * one, centre * two]
    for step_y in (-1, 0, 1):
        side = [moved(x, 0, step_y) for x in (one, two)]
        if step_y:
            pairs = {
                step_y: [moved(x, 0, step_y) for x in plus],
                -step_y: [moved(x, 0, step_y) for x in minus],
            }
            for c in (0, 1):
                out[c] = out[c] + weights[0, step_y] * side[c]
        for step_x in (-1, 1):
            fields = pairs[step_x] if step_y else side
            for c in (0, 1):
                out[c] = out[c] + weights[step_x, step_y] * moved(fields[c], step_x, 0)
    return out


def column_kernel(wide_ref, own_ref, sums_ref, up_ref, down_ref):
    levels = wide_ref.shape[0] - FIELDS
    rows, cols = own_ref.shape[1:]
    friction = wide_ref[levels]
    source = (wide_ref[levels + 1], wide_ref[levels + 2])
    obs = wide_ref[levels + 3]
    inverse_diag = wide_ref[levels + 4]
    gradient = wide_ref[levels + 5]
    warm_start = wide_ref[levels + 6]
    outside = jnp.where(wide_ref[0] > 0.0, 0.0, 1.0)
    through = vertical(wide_ref, friction, outside, up_ref, down_ref)
    back = couplings(wide_ref, up_ref, down_ref)
    forth = {(dx, dy): moved(back[-dx, -dy], dx, dy) for dx, dy in back}

    def hessian(q):
        surface = spread(forth, through, source[0] * q, source[1] * q)
        basal = spread(back, through, obs * surface[0], obs * surface[1])
        beside = moved(q, 1, 0) + moved(q, -1, 0) + moved(q, 0, 1) + moved(q, 0, -1)
        smooth = reg_gamma * (q + reg_smooth * (4.0 * q - beside))
        return source[0] * basal[0] + source[1] * basal[1] + smooth

    residual = gradient - hessian(warm_start)
    direction = inverse_diag * residual
    image = hessian(direction)
    second = inverse_diag * image
    second_image = hessian(second)

    def own(field):
        return field[HALO : HALO + rows, HALO : HALO + cols]

    kept = [own(x) for x in (residual, direction, image, second, second_image)]
    for index, field in enumerate(kept):
        own_ref[index] = field
    residual, direction, image, second, second_image = kept
    parts = (residual * direction, direction * image, second * image, second * second_image)
    for index, part in enumerate(parts):
        sums_ref[index : index + 1] = jnp.sum(part, axis=0, keepdims=True)


def exchanged(block, axis, dim, width):
    count = lax.axis_size(axis)
    forward = [(i, i + 1) for i in range(count - 1)]
    backward = [(target, source) for source, target in forward]
    low = lax.ppermute(
        lax.slice_in_dim(block, block.shape[dim] - width, None, axis=dim), axis, forward
    )
    high = lax.ppermute(lax.slice_in_dim(block, 0, width, axis=dim), axis, backward)
    return jnp.concatenate([low, block, high], axis=dim)


def summed(values):
    for axis in ("gx", "gy"):
        count = lax.axis_size(axis)
        step = 1
        while step < count:
            pairs = [(i, i ^ step) for i in range(count)]
            values = values + lax.ppermute(values, axis, pairs)
            step *= 2
    return values


def on_device(
    gradient, warm_start, viscosity, friction_coef, slide_dir, obs_weight, ice_mask, grounded
):
    levels, rows, cols = viscosity.shape
    ice_float = ice_mask.astype(jnp.float32)
    ground_float = grounded.astype(jnp.float32)
    friction = ground_float * friction_coef
    source = (ice_float * ground_float * friction_coef)[None] * slide_dir
    obs = ice_float * obs_weight
    inverse_diag = 1.0 / (
        reg_gamma * (1.0 + 4.0 * reg_smooth)
        + diag_scale * ice_float * ground_float * friction_coef * friction_coef
    )
    columns = jnp.stack(
        [friction, source[0], source[1], obs, inverse_diag, gradient, warm_start]
    )
    stacked = jnp.concatenate([viscosity, columns], axis=0)
    wide = exchanged(stacked, "gy", 2, HALO)
    wide = exchanged(wide, "gx", 1, HALO)
    span_x = round_up(rows + 2 * HALO, 8)
    span_y = round_up(cols + 2 * HALO, 128)
    wide = jnp.pad(
        wide, ((0, 0), (0, span_x - rows - 2 * HALO), (0, span_y - cols - 2 * HALO))
    )
    own, sums = pl.pallas_call(
        column_kernel,
        out_shape=(
            jax.ShapeDtypeStruct((5, rows, cols), jnp.float32),
            jax.ShapeDtypeStruct((4, cols), jnp.float32),
        ),
        scratch_shapes=[pltpu.VMEM((levels, span_x, span_y), jnp.float32)] * 2,
        name="columns",
    )(wide)
    residual, direction, image, second, second_image = own
    norm_now, curve, cross, second_curve = summed(jnp.sum(sums, axis=1))
    first_step = norm_now / curve
    norm_next = first_step * first_step * cross - norm_now
    ratio = norm_next / norm_now
    grow = 1.0 + ratio
    next_curve = (
        grow * grow * curve
        - 2.0 * grow * first_step * cross
        + first_step * first_step * second_curve
    )
    next_step = norm_next / next_curve
    solution = (
        warm_start
        + first_step * direction
        + next_step * (grow * direction - first_step * second)
    )
    residual = (
        residual - first_step * image - next_step * (grow * image - first_step * second_image)
    )
    return (solution, residual)


def solution(mesh):
    return jax.shard_map(
        on_device,
        mesh=mesh,
        in_specs=(
            P("gx", "gy"),
            P("gx", "gy"),
            P(None, "gx", "gy"),
            P("gx", "gy"),
            P(None, "gx", "gy"),
            P("gx", "gy"),
            P("gx", "gy"),
            P("gx", "gy"),
        ),
        out_specs=(P("gx", "gy"), P("gx", "gy")),
        check_vma=False,
    )
```

```python
import jax
import jax.numpy as jnp
from jax import lax
from jax.experimental import pallas as pl
from jax.experimental.pallas import tpu as pltpu
from jax.sharding import PartitionSpec as P

vert_coupling = 128.0
sink_rate = 0.0625
bed_drag = 0.5
offset_weight = 0.0019
cross_share = 0.5
reg_gamma = 0.02
reg_smooth = 1.0
diag_scale = 0.003

HALO = 6
FIELDS = 7
LANES = 128
SLOTS = LANES // HALO
UNROLL = 4


def moved(block, step_x, step_y):
    if step_y:
        block = pltpu.roll(block, (-step_y) % block.shape[1], 1)
    if step_x:
        block = pltpu.roll(block, (-step_x) % block.shape[0], 0)
    return block


def turned(block, amount):
    amount %= LANES
    return pltpu.roll(block, amount, 1) if amount else block


def field_kernel(gradient, warm_start, friction_coef, slide, obs_weight, ice, grounded, out_ref):
    ice_float = ice[...].astype(jnp.float32)
    ground_float = grounded[...].astype(jnp.float32)
    coef = friction_coef[...]
    source = ice_float * ground_float * coef
    out_ref[0] = ground_float * coef
    out_ref[1] = source * slide[0]
    out_ref[2] = source * slide[1]
    out_ref[3] = ice_float * obs_weight[...]
    out_ref[4] = 1.0 / (
        reg_gamma * (1.0 + 4.0 * reg_smooth)
        + diag_scale * ice_float * ground_float * coef * coef
    )
    out_ref[5] = gradient[...]
    out_ref[6] = warm_start[...]


def pack_kernel(*refs):
    layers, fields = refs[0:3], refs[3:6]
    to_low, to_high = refs[6:8]
    levels, rows, cols = layers[0].shape
    lane = lax.broadcasted_iota(jnp.int32, (rows, LANES), 1)
    for t in range(3):
        for group in range(0, levels + FIELDS, SLOTS):
            first = jnp.zeros((rows, LANES), jnp.float32)
            last = first
            for z in range(group, min(group + SLOTS, levels + FIELDS)):
                ref, index = (layers[t], z) if z < levels else (fields[t], z - levels)
                at = HALO * (z - group)
                here = (lane >= at) & (lane < at + HALO)
                first = jnp.where(here, turned(ref[index, :, :LANES], at), first)
                shift = at - (LANES - HALO)
                last = jnp.where(here, turned(ref[index, :, cols - LANES :], shift), last)
            place = (group // SLOTS) * LANES
            to_low[t * rows : (t + 1) * rows, place : place + LANES] = first
            to_high[t * rows : (t + 1) * rows, place : place + LANES] = last


def assemble(layers, fields, from_low, from_high, wide_ref):
    levels, rows, cols = layers[0].shape
    lane = lax.broadcasted_iota(jnp.int32, (rows, LANES), 1)
    for z in range(levels + FIELDS):
        at = HALO * (z % SLOTS)
        place = (z // SLOTS) * LANES
        for t in range(3):
            ref, index = (layers[t], z) if z < levels else (fields[t], z - levels)
            band = slice(t * rows, (t + 1) * rows)
            wide_ref[z, band, :cols] = ref[index]
            high = turned(from_high[band, place : place + LANES], -at)
            low = turned(from_low[band, place : place + LANES], LANES - HALO - at)
            edge = jnp.where(lane < HALO, high, jnp.where(lane >= LANES - HALO, low, 0.0))
            wide_ref[z, band, cols:] = edge


def vertical(wide_ref, tops, heavy_tops, bed_ref, heavy_bed):
    levels = wide_ref.shape[0] - FIELDS
    half = 0.5 * vert_coupling
    friction = bed_drag * wide_ref[levels]
    inside = jnp.where(wide_ref[0] > 0.0, 1.0, 0.0)
    outside = 1.0 - inside
    up_ref = tops[1]

    def eliminate(k, carry):
        low, high, up_here, down_here = carry
        up_next = wide_ref[k + 1] + outside
        link = half * (up_here + up_next)
        ratio = link / (link + low)
        up_ref[k] = ratio
        low = sink_rate * up_next + ratio * low
        m = levels - 2 - k
        down_next = wide_ref[m] + outside
        link = half * (down_here + down_next)
        ratio = link / (link + high)
        bed_ref[m + 2] = ratio
        high = sink_rate * down_next + ratio * high
        return low, high, up_next, down_next

    up_here = wide_ref[0] + outside
    down_here = wide_ref[levels - 1] + outside
    low = sink_rate * up_here + friction
    high = sink_rate * down_here
    low, high, _, _ = lax.fori_loop(0, levels - 1, eliminate, (low, high, up_here, down_here))

    def keep(k, top, m, bed):
        heavy = top * wide_ref[k]
        for index, step in enumerate((-1, 0, 1)):
            tops[index][k] = moved(top, step, 0)
            heavy_tops[index][k] = moved(heavy, step, 0)
        bed_ref[m + 1] = bed
        heavy_bed[m + 1] = bed * wide_ref[m]

    def substitute(k, carry):
        top, bed = carry
        m = levels - 2 - k
        top = up_ref[m] * top
        bed = bed_ref[k + 2] * bed
        keep(m, top, k + 1, bed)
        return top, bed

    top = inside / low
    bed = inside / (high + friction)
    keep(levels - 1, top, 0, bed)
    zero = jnp.zeros(bed.shape, jnp.float32)
    for ref in (bed_ref, heavy_bed):
        ref[0] = zero
        ref[levels + 1] = zero
    top, bed = lax.fori_loop(0, levels - 1, substitute, (top, bed))
    return top


def couplings(levels, rows, tops, heavy_tops, bed_ref, heavy_bed):
    span_x, span_y = bed_ref.shape[1:]
    offsets = [(dx, dy) for dx in (-1, 0, 1) for dy in (-1, 0, 1) if dx or dy]
    unroll = UNROLL if levels % UNROLL == 0 else 1
    bands = []
    for start in range(0, span_x, rows):
        band = slice(start, start + rows)

        def layer(k, sums):
            reach = {}
            here, sides = bed_ref[k + 1, band], bed_ref[k, band] + bed_ref[k + 2, band]
            v_here = heavy_bed[k + 1, band]
            v_sides = heavy_bed[k, band] + heavy_bed[k + 2, band]
            for count in (1, 2):
                near = offset_weight * 0.5 / count
                far = offset_weight * 0.5 / (count + 1)
                plain, heavy = near * here + far * sides, near * v_here + far * v_sides
                for step_y in (-1, 0, 1):
                    if count == 1 or step_y:
                        reach[count, step_y] = (moved(plain, 0, -step_y), moved(heavy, 0, -step_y))
            out = []
            for (step_x, step_y), total in zip(offsets, sums):
                plain, heavy = reach[abs(step_x) + abs(step_y), step_y]
                top, v_top = tops[step_x + 1][k, band], heavy_tops[step_x + 1][k, band]
                out.append(total + (v_top * plain + top * heavy))
            return tuple(out)

        def layers(block, sums):
            for i in range(unroll):
                sums = layer(block * unroll + i, sums)
            return sums

        zero = jnp.zeros((rows, span_y), jnp.float32)
        bands.append(lax.fori_loop(0, levels // unroll, layers, (zero,) * len(offsets)))
    return {
        (dx, dy): moved(jnp.concatenate([band[i] for band in bands], axis=0), 0, dy)
        for i, (dx, dy) in enumerate(offsets)
    }


def spread(weights, centre, one, two):
    plus = (one + cross_share * two, two + cross_share * one)
    minus = (one - cross_share * two, two - cross_share * one)
    out = [centre * one, centre * two]
    for step_y in (-1, 0, 1):
        side = [moved(x, 0, step_y) for x in (one, two)]
        if step_y:
            pairs = {
                step_y: [moved(x, 0, step_y) for x in plus],
                -step_y: [moved(x, 0, step_y) for x in minus],
            }
            for c in (0, 1):
                out[c] = out[c] + weights[0, step_y] * side[c]
        for step_x in (-1, 1):
            fields = pairs[step_x] if step_y else side
            for c in (0, 1):
                out[c] = out[c] + weights[step_x, step_y] * moved(fields[c], step_x, 0)
    return out


def column_kernel(*refs):
    layers, fields, (from_low, from_high) = refs[0:3], refs[3:6], refs[6:8]
    own_ref, sums_ref, wide_ref = refs[8:11]
    tops, heavy_tops, (bed_ref, heavy_bed) = refs[11:14], refs[14:17], refs[17:19]
    levels, rows, cols = layers[0].shape
    assemble(layers, fields, from_low, from_high, wide_ref)
    through = vertical(wide_ref, tops, heavy_tops, bed_ref, heavy_bed)
    back = couplings(levels, rows, tops, heavy_tops, bed_ref, heavy_bed)
    forth = {(dx, dy): moved(back[-dx, -dy], dx, dy) for dx, dy in back}
    source = (wide_ref[levels + 1], wide_ref[levels + 2])
    obs, inverse_diag = wide_ref[levels + 3], wide_ref[levels + 4]
    gradient, warm_start = wide_ref[levels + 5], wide_ref[levels + 6]

    def hessian(q):
        surface = spread(forth, through, source[0] * q, source[1] * q)
        basal = spread(back, through, obs * surface[0], obs * surface[1])
        beside = moved(q, 1, 0) + moved(q, -1, 0) + moved(q, 0, 1) + moved(q, 0, -1)
        smooth = reg_gamma * (q + reg_smooth * (4.0 * q - beside))
        return source[0] * basal[0] + source[1] * basal[1] + smooth

    residual = gradient - hessian(warm_start)
    direction = inverse_diag * residual
    image = hessian(direction)
    second = inverse_diag * image
    second_image = hessian(second)
    kept = [x[:rows, :cols] for x in (residual, direction, image, second, second_image)]
    for index, field in enumerate(kept):
        own_ref[index] = field
    residual, direction, image, second, second_image = kept
    parts = (residual * direction, direction * image, second * image, second * second_image)
    rows_of_sums = []
    for part in parts:
        total = jnp.sum(part, axis=0, keepdims=True)
        rows_of_sums.append(sum(total[:, i : i + LANES] for i in range(0, cols, LANES)))
    sums = jnp.concatenate(rows_of_sums, axis=0)
    for device in range(sums_ref.shape[0]):
        sums_ref[device] = sums


def finish_kernel(sums_ref, own_ref, warm_start, solution_ref, residual_ref):
    sums = jnp.sum(jnp.sum(sums_ref[...], axis=0), axis=1, keepdims=True)
    norm_now, curve, cross, second_curve = (sums[i : i + 1] for i in range(4))
    residual, direction, image, second, second_image = (own_ref[i] for i in range(5))
    first_step = norm_now / curve
    norm_next = first_step * first_step * cross - norm_now
    grow = 1.0 + norm_next / norm_now
    next_curve = (
        grow * grow * curve
        - 2.0 * grow * first_step * cross
        + first_step * first_step * second_curve
    )
    next_step = norm_next / next_curve
    solution_ref[...] = (
        warm_start[...]
        + first_step * direction
        + next_step * (grow * direction - first_step * second)
    )
    residual_ref[...] = (
        residual - first_step * image - next_step * (grow * image - first_step * second_image)
    )


def neighbours(axis):
    forward = [(i, i + 1) for i in range(lax.axis_size(axis) - 1)]
    return forward, [(target, source) for source, target in forward]


def on_device(
    gradient, warm_start, viscosity, friction_coef, slide_dir, obs_weight, ice_mask, grounded
):
    levels, rows, cols = viscosity.shape
    forward, backward = neighbours("gx")
    layers = (
        viscosity,
        lax.ppermute(viscosity, "gx", backward),
        lax.ppermute(viscosity, "gx", forward),
    )
    own_fields = pl.pallas_call(
        field_kernel,
        out_shape=jax.ShapeDtypeStruct((FIELDS, rows, cols), jnp.float32),
        name="fields",
    )(gradient, warm_start, friction_coef, slide_dir, obs_weight, ice_mask, grounded)
    fields = (
        own_fields,
        lax.ppermute(own_fields, "gx", backward),
        lax.ppermute(own_fields, "gx", forward),
    )
    packed = jax.ShapeDtypeStruct(
        (3 * rows, -(-(levels + FIELDS) // SLOTS) * LANES), jnp.float32
    )
    to_low, to_high = pl.pallas_call(pack_kernel, out_shape=(packed, packed), name="pack")(
        *layers, *fields
    )
    forward, backward = neighbours("gy")
    from_high = lax.ppermute(to_low, "gy", backward)
    from_low = lax.ppermute(to_high, "gy", forward)
    devices = lax.axis_size("gx") * lax.axis_size("gy")
    span = (3 * rows, cols + LANES)
    own, sums = pl.pallas_call(
        column_kernel,
        out_shape=(
            jax.ShapeDtypeStruct((5, rows, cols), jnp.float32),
            jax.ShapeDtypeStruct((devices, 4, LANES), jnp.float32),
        ),
        scratch_shapes=[pltpu.VMEM((levels + FIELDS,) + span, jnp.float32)]
        + [pltpu.VMEM((levels,) + span, jnp.float32)] * 6
        + [pltpu.VMEM((levels + 2,) + span, jnp.float32)] * 2,
        name="columns",
    )(*layers, *fields, from_low, from_high)
    sums = lax.all_to_all(sums, ("gx", "gy"), 0, 0)
    return pl.pallas_call(
        finish_kernel,
        out_shape=(jax.ShapeDtypeStruct((rows, cols), jnp.float32),) * 2,
        name="finish",
    )(sums, own, warm_start)


def solution(mesh):
    return jax.shard_map(
        on_device,
        mesh=mesh,
        in_specs=(
            P("gx", "gy"),
            P("gx", "gy"),
            P(None, "gx", "gy"),
            P("gx", "gy"),
            P(None, "gx", "gy"),
            P("gx", "gy"),
            P("gx", "gy"),
            P("gx", "gy"),
        ),
        out_specs=(P("gx", "gy"), P("gx", "gy")),
        check_vma=False,
    )
```

```python
import jax
import jax.numpy as jnp
from jax import lax
from jax.experimental import pallas as pl
from jax.experimental.pallas import tpu as pltpu
from jax.sharding import PartitionSpec as P

vert_coupling = 128.0
sink_rate = 0.0625
bed_drag = 0.5
offset_weight = 0.0019
cross_share = 0.5
reg_gamma = 0.02
reg_smooth = 1.0
diag_scale = 0.003

HALO = 6
FIELDS = 7
LANES = 128
SLOTS = LANES // HALO
UNROLL = 4


def moved(block, step_x, step_y):
    if step_y:
        block = pltpu.roll(block, (-step_y) % block.shape[1], 1)
    if step_x:
        block = pltpu.roll(block, (-step_x) % block.shape[0], 0)
    return block


def turned(block, amount):
    amount %= LANES
    return pltpu.roll(block, amount, 1) if amount else block


def field_kernel(
    visc, gradient, warm_start, friction_coef, slide, obs_weight, ice, grounded, *out_refs
):
    own_ref, to_low, to_high = out_refs
    levels, rows, _ = visc.shape
    ice_float = ice[...].astype(jnp.float32)
    ground_float = grounded[...].astype(jnp.float32)
    coef = friction_coef[...]
    source = ice_float * ground_float * coef
    own_ref[0] = ground_float * coef
    own_ref[1] = source * slide[0]
    own_ref[2] = source * slide[1]
    own_ref[3] = ice_float * obs_weight[...]
    own_ref[4] = 1.0 / (
        reg_gamma * (1.0 + 4.0 * reg_smooth)
        + diag_scale * ice_float * ground_float * coef * coef
    )
    own_ref[5] = gradient[...]
    own_ref[6] = warm_start[...]
    tiles = [visc[z] for z in range(levels)] + [own_ref[z] for z in range(FIELDS)]
    for z, tile in enumerate(tiles):
        to_low[HALO * z : HALO * z + rows] = tile
    for z in range(levels + FIELDS - 1, -1, -1):
        to_high[HALO * z : HALO * z + rows] = tiles[z]


def tiles_of(visc, own, from_low, from_high, z, lanes):
    levels, rows, _ = visc.shape
    ref, index = (visc, z) if z < levels else (own, z - levels)
    band = slice(HALO * z, HALO * z + rows)
    own_tile, high, low = ref[index, :, lanes], from_high[band, lanes], from_low[band, lanes]
    row = lax.broadcasted_iota(jnp.int32, own_tile.shape, 0)
    return (
        own_tile,
        jnp.where(row < HALO, high, 0.0),
        jnp.where(row >= rows - HALO, low, 0.0),
    )


def pack_kernel(visc, own, row_low, row_high, to_low, to_high):
    levels, rows, cols = visc.shape
    lane = lax.broadcasted_iota(jnp.int32, (rows, LANES), 1)
    zero = jnp.zeros((rows, LANES), jnp.float32)
    for group in range(0, levels + FIELDS, SLOTS):
        first, last = [zero] * 3, [zero] * 3
        for z in range(group, min(group + SLOTS, levels + FIELDS)):
            at = HALO * (z - group)
            here = (lane >= at) & (lane < at + HALO)
            shift = at - (LANES - HALO)
            left = tiles_of(visc, own, row_low, row_high, z, slice(0, LANES))
            right = tiles_of(visc, own, row_low, row_high, z, slice(cols - LANES, cols))
            for t in range(3):
                first[t] = jnp.where(here, turned(left[t], at), first[t])
                last[t] = jnp.where(here, turned(right[t], shift), last[t])
        place = (group // SLOTS) * LANES
        for t in range(3):
            to_low[t * rows : (t + 1) * rows, place : place + LANES] = first[t]
            to_high[t * rows : (t + 1) * rows, place : place + LANES] = last[t]


def assemble(visc, own, row_low, row_high, from_low, from_high, wide_ref):
    levels, rows, cols = visc.shape
    lane = lax.broadcasted_iota(jnp.int32, (rows, LANES), 1)
    for z in range(levels + FIELDS):
        at = HALO * (z % SLOTS)
        place = (z // SLOTS) * LANES
        tiles = tiles_of(visc, own, row_low, row_high, z, slice(0, cols))
        for t in range(3):
            band = slice(t * rows, (t + 1) * rows)
            wide_ref[z, band, :cols] = tiles[t]
            high = turned(from_high[band, place : place + LANES], -at)
            low = turned(from_low[band, place : place + LANES], LANES - HALO - at)
            edge = jnp.where(lane < HALO, high, jnp.where(lane >= LANES - HALO, low, 0.0))
            wide_ref[z, band, cols:] = edge


def vertical(wide_ref, tops, heavy_tops, bed_ref, heavy_bed):
    levels = wide_ref.shape[0] - FIELDS
    half = 0.5 * vert_coupling
    friction = bed_drag * wide_ref[levels]
    inside = jnp.where(wide_ref[0] > 0.0, 1.0, 0.0)
    outside = 1.0 - inside
    up_ref = tops[1]

    def eliminate(k, carry):
        low, high, up_here, down_here = carry
        up_next = wide_ref[k + 1] + outside
        link = half * (up_here + up_next)
        ratio = link / (link + low)
        up_ref[k] = ratio
        low = sink_rate * up_next + ratio * low
        m = levels - 2 - k
        down_next = wide_ref[m] + outside
        link = half * (down_here + down_next)
        ratio = link / (link + high)
        bed_ref[m + 2] = ratio
        high = sink_rate * down_next + ratio * high
        return low, high, up_next, down_next

    up_here = wide_ref[0] + outside
    down_here = wide_ref[levels - 1] + outside
    low = sink_rate * up_here + friction
    high = sink_rate * down_here
    low, high, _, _ = lax.fori_loop(0, levels - 1, eliminate, (low, high, up_here, down_here))

    def keep(k, top, m, bed):
        heavy = top * wide_ref[k]
        for index, step in enumerate((-1, 0, 1)):
            tops[index][k] = moved(top, step, 0)
            heavy_tops[index][k] = moved(heavy, step, 0)
        bed_ref[m + 1] = bed
        heavy_bed[m + 1] = bed * wide_ref[m]

    def substitute(k, carry):
        top, bed = carry
        m = levels - 2 - k
        top = up_ref[m] * top
        bed = bed_ref[k + 2] * bed
        keep(m, top, k + 1, bed)
        return top, bed

    top = inside / low
    bed = inside / (high + friction)
    keep(levels - 1, top, 0, bed)
    zero = jnp.zeros(bed.shape, jnp.float32)
    for ref in (bed_ref, heavy_bed):
        ref[0] = zero
        ref[levels + 1] = zero
    top, bed = lax.fori_loop(0, levels - 1, substitute, (top, bed))
    return top


def couplings(levels, rows, tops, heavy_tops, bed_ref, heavy_bed):
    span_x, span_y = bed_ref.shape[1:]
    offsets = [(dx, dy) for dx in (-1, 0, 1) for dy in (-1, 0, 1) if dx or dy]
    unroll = UNROLL if levels % UNROLL == 0 else 1
    bands = []
    for start in range(0, span_x, rows):
        band = slice(start, start + rows)

        def layer(k, sums):
            reach = {}
            here, sides = bed_ref[k + 1, band], bed_ref[k, band] + bed_ref[k + 2, band]
            v_here = heavy_bed[k + 1, band]
            v_sides = heavy_bed[k, band] + heavy_bed[k + 2, band]
            for count in (1, 2):
                near = offset_weight * 0.5 / count
                far = offset_weight * 0.5 / (count + 1)
                plain, heavy = near * here + far * sides, near * v_here + far * v_sides
                for step_y in (-1, 0, 1):
                    if count == 1 or step_y:
                        reach[count, step_y] = (moved(plain, 0, -step_y), moved(heavy, 0, -step_y))
            out = []
            for (step_x, step_y), total in zip(offsets, sums):
                plain, heavy = reach[abs(step_x) + abs(step_y), step_y]
                top, v_top = tops[step_x + 1][k, band], heavy_tops[step_x + 1][k, band]
                out.append(total + (v_top * plain + top * heavy))
            return tuple(out)

        def layers(block, sums):
            for i in range(unroll):
                sums = layer(block * unroll + i, sums)
            return sums

        zero = jnp.zeros((rows, span_y), jnp.float32)
        bands.append(lax.fori_loop(0, levels // unroll, layers, (zero,) * len(offsets)))
    return {
        (dx, dy): moved(jnp.concatenate([band[i] for band in bands], axis=0), 0, dy)
        for i, (dx, dy) in enumerate(offsets)
    }


def spread(weights, centre, one, two):
    plus = (one + cross_share * two, two + cross_share * one)
    minus = (one - cross_share * two, two - cross_share * one)
    out = [centre * one, centre * two]
    for step_y in (-1, 0, 1):
        side = [moved(x, 0, step_y) for x in (one, two)]
        if step_y:
            pairs = {
                step_y: [moved(x, 0, step_y) for x in plus],
                -step_y: [moved(x, 0, step_y) for x in minus],
            }
            for c in (0, 1):
                out[c] = out[c] + weights[0, step_y] * side[c]
        for step_x in (-1, 1):
            fields = pairs[step_x] if step_y else side
            for c in (0, 1):
                out[c] = out[c] + weights[step_x, step_y] * moved(fields[c], step_x, 0)
    return out


def column_kernel(*refs):
    own_ref, sums_ref, wide_ref = refs[6:9]
    tops, heavy_tops, (bed_ref, heavy_bed) = refs[9:12], refs[12:15], refs[15:17]
    levels, rows, cols = refs[0].shape
    assemble(*refs[0:6], wide_ref)
    through = vertical(wide_ref, tops, heavy_tops, bed_ref, heavy_bed)
    back = couplings(levels, rows, tops, heavy_tops, bed_ref, heavy_bed)
    forth = {(dx, dy): moved(back[-dx, -dy], dx, dy) for dx, dy in back}
    source = (wide_ref[levels + 1], wide_ref[levels + 2])
    obs, inverse_diag = wide_ref[levels + 3], wide_ref[levels + 4]
    gradient, warm_start = wide_ref[levels + 5], wide_ref[levels + 6]

    def hessian(q):
        surface = spread(forth, through, source[0] * q, source[1] * q)
        basal = spread(back, through, obs * surface[0], obs * surface[1])
        beside = moved(q, 1, 0) + moved(q, -1, 0) + moved(q, 0, 1) + moved(q, 0, -1)
        smooth = reg_gamma * (q + reg_smooth * (4.0 * q - beside))
        return source[0] * basal[0] + source[1] * basal[1] + smooth

    residual = gradient - hessian(warm_start)
    direction = inverse_diag * residual
    image = hessian(direction)
    second = inverse_diag * image
    second_image = hessian(second)
    kept = [x[:rows, :cols] for x in (residual, direction, image, second, second_image)]
    for index, field in enumerate(kept):
        own_ref[index] = field
    residual, direction, image, second, second_image = kept
    parts = (residual * direction, direction * image, second * image, second * second_image)
    rows_of_sums = []
    for part in parts:
        total = jnp.sum(part, axis=0, keepdims=True)
        rows_of_sums.append(sum(total[:, i : i + LANES] for i in range(0, cols, LANES)))
    sums = jnp.concatenate(rows_of_sums, axis=0)
    for device in range(sums_ref.shape[0]):
        sums_ref[device] = sums


def finish_kernel(sums_ref, own_ref, warm_start, solution_ref, residual_ref):
    sums = jnp.sum(jnp.sum(sums_ref[...], axis=0), axis=1, keepdims=True)
    norm_now, curve, cross, second_curve = (sums[i : i + 1] for i in range(4))
    residual, direction, image, second, second_image = (own_ref[i] for i in range(5))
    first_step = norm_now / curve
    norm_next = first_step * first_step * cross - norm_now
    grow = 1.0 + norm_next / norm_now
    next_curve = (
        grow * grow * curve
        - 2.0 * grow * first_step * cross
        + first_step * first_step * second_curve
    )
    next_step = norm_next / next_curve
    solution_ref[...] = (
        warm_start[...]
        + first_step * direction
        + next_step * (grow * direction - first_step * second)
    )
    residual_ref[...] = (
        residual - first_step * image - next_step * (grow * image - first_step * second_image)
    )


def neighbours(axis):
    forward = [(i, i + 1) for i in range(lax.axis_size(axis) - 1)]
    return forward, [(target, source) for source, target in forward]


def on_device(
    gradient, warm_start, viscosity, friction_coef, slide_dir, obs_weight, ice_mask, grounded
):
    levels, rows, cols = viscosity.shape
    sent = jax.ShapeDtypeStruct((-(-(HALO * (levels + FIELDS) + rows) // 8) * 8, cols), jnp.float32)
    fields, to_low, to_high = pl.pallas_call(
        field_kernel,
        out_shape=(jax.ShapeDtypeStruct((FIELDS, rows, cols), jnp.float32), sent, sent),
        name="fields",
    )(viscosity, gradient, warm_start, friction_coef, slide_dir, obs_weight, ice_mask, grounded)
    forward, backward = neighbours("gx")
    row_high = lax.ppermute(to_low, "gx", backward)
    row_low = lax.ppermute(to_high, "gx", forward)
    packed = jax.ShapeDtypeStruct(
        (3 * rows, -(-(levels + FIELDS) // SLOTS) * LANES), jnp.float32
    )
    pieces = (viscosity, fields, row_low, row_high)
    to_low, to_high = pl.pallas_call(pack_kernel, out_shape=(packed, packed), name="pack")(*pieces)
    forward, backward = neighbours("gy")
    from_high = lax.ppermute(to_low, "gy", backward)
    from_low = lax.ppermute(to_high, "gy", forward)
    devices = lax.axis_size("gx") * lax.axis_size("gy")
    span = (3 * rows, cols + LANES)
    own, sums = pl.pallas_call(
        column_kernel,
        out_shape=(
            jax.ShapeDtypeStruct((5, rows, cols), jnp.float32),
            jax.ShapeDtypeStruct((devices, 4, LANES), jnp.float32),
        ),
        scratch_shapes=[pltpu.VMEM((levels + FIELDS,) + span, jnp.float32)]
        + [pltpu.VMEM((levels,) + span, jnp.float32)] * 6
        + [pltpu.VMEM((levels + 2,) + span, jnp.float32)] * 2,
        name="columns",
    )(*pieces, from_low, from_high)
    sums = lax.all_to_all(sums, ("gx", "gy"), 0, 0)
    return pl.pallas_call(
        finish_kernel,
        out_shape=(jax.ShapeDtypeStruct((rows, cols), jnp.float32),) * 2,
        name="finish",
    )(sums, own, warm_start)


def solution(mesh):
    return jax.shard_map(
        on_device,
        mesh=mesh,
        in_specs=(
            P("gx", "gy"),
            P("gx", "gy"),
            P(None, "gx", "gy"),
            P("gx", "gy"),
            P(None, "gx", "gy"),
            P("gx", "gy"),
            P("gx", "gy"),
            P("gx", "gy"),
        ),
        out_specs=(P("gx", "gy"), P("gx", "gy")),
        check_vma=False,
    )
```

```python
import jax
import jax.numpy as jnp
from jax import lax
from jax.experimental import pallas as pl
from jax.experimental.pallas import tpu as pltpu
from jax.sharding import PartitionSpec as P

vert_coupling = 128.0
sink_rate = 0.0625
bed_drag = 0.5
offset_weight = 0.0019
cross_share = 0.5
reg_gamma = 0.02
reg_smooth = 1.0
diag_scale = 0.003

HALO = 6
FIELDS = 7
LANES = 128
SLOTS = LANES // HALO
UNROLL = 4


def moved(block, step_x, step_y):
    if step_y:
        block = pltpu.roll(block, (-step_y) % block.shape[1], 1)
    if step_x:
        block = pltpu.roll(block, (-step_x) % block.shape[0], 0)
    return block


def turned(block, amount):
    amount %= LANES
    return pltpu.roll(block, amount, 1) if amount else block


def field_kernel(
    visc, gradient, warm_start, friction_coef, slide, obs_weight, ice, grounded, *out_refs
):
    own_ref, to_low, to_high, first_ref, last_ref = out_refs
    levels, rows, cols = visc.shape
    ice_float = ice[...].astype(jnp.float32)
    ground_float = grounded[...].astype(jnp.float32)
    coef = friction_coef[...]
    source = ice_float * ground_float * coef
    own_ref[0] = ground_float * coef
    own_ref[1] = source * slide[0]
    own_ref[2] = source * slide[1]
    own_ref[3] = ice_float * obs_weight[...]
    own_ref[4] = 1.0 / (
        reg_gamma * (1.0 + 4.0 * reg_smooth)
        + diag_scale * ice_float * ground_float * coef * coef
    )
    own_ref[5] = gradient[...]
    own_ref[6] = warm_start[...]
    tiles = [visc[z] for z in range(levels)] + [own_ref[z] for z in range(FIELDS)]
    for z, tile in enumerate(tiles):
        to_low[HALO * z : HALO * z + rows] = tile
    for z in range(levels + FIELDS - 1, -1, -1):
        to_high[HALO * z : HALO * z + rows] = tiles[z]
    lane = lax.broadcasted_iota(jnp.int32, (rows, LANES), 1)
    for group in range(0, levels + FIELDS, SLOTS):
        first = jnp.zeros((rows, LANES), jnp.float32)
        last = first
        for z in range(group, min(group + SLOTS, levels + FIELDS)):
            at = HALO * (z - group)
            here = (lane >= at) & (lane < at + HALO)
            first = jnp.where(here, turned(tiles[z][:, :LANES], at), first)
            shift = at - (LANES - HALO)
            last = jnp.where(here, turned(tiles[z][:, cols - LANES :], shift), last)
        place = (group // SLOTS) * LANES
        first_ref[:, place : place + LANES] = first
        last_ref[:, place : place + LANES] = last


def tiles_of(visc, own, from_low, from_high, z, lanes):
    levels, rows, _ = visc.shape
    ref, index = (visc, z) if z < levels else (own, z - levels)
    band = slice(HALO * z, HALO * z + rows)
    own_tile, high, low = ref[index, :, lanes], from_high[band, lanes], from_low[band, lanes]
    row = lax.broadcasted_iota(jnp.int32, own_tile.shape, 0)
    return (
        own_tile,
        jnp.where(row < HALO, high, 0.0),
        jnp.where(row >= rows - HALO, low, 0.0),
    )


def assemble(visc, own, row_low, row_high, edges, wide_ref):
    levels, rows, cols = visc.shape
    lane = lax.broadcasted_iota(jnp.int32, (rows, LANES), 1)
    for z in range(levels + FIELDS):
        at = HALO * (z % SLOTS)
        place = (z // SLOTS) * LANES
        tiles = tiles_of(visc, own, row_low, row_high, z, slice(0, cols))
        for t in range(3):
            band = slice(t * rows, (t + 1) * rows)
            wide_ref[z, band, :cols] = tiles[t]
            low = turned(edges[t][0, :, place : place + LANES], LANES - HALO - at)
            high = turned(edges[t][1, :, place : place + LANES], -at)
            edge = jnp.where(lane < HALO, high, jnp.where(lane >= LANES - HALO, low, 0.0))
            wide_ref[z, band, cols:] = edge


def vertical(wide_ref, tops, heavy_tops, bed_ref, heavy_bed):
    levels = wide_ref.shape[0] - FIELDS
    half = 0.5 * vert_coupling
    friction = bed_drag * wide_ref[levels]
    inside = jnp.where(wide_ref[0] > 0.0, 1.0, 0.0)
    outside = 1.0 - inside
    up_ref = tops[1]

    def eliminate(k, carry):
        low, high, up_here, down_here = carry
        up_next = wide_ref[k + 1] + outside
        link = half * (up_here + up_next)
        ratio = link / (link + low)
        up_ref[k] = ratio
        low = sink_rate * up_next + ratio * low
        m = levels - 2 - k
        down_next = wide_ref[m] + outside
        link = half * (down_here + down_next)
        ratio = link / (link + high)
        bed_ref[m + 2] = ratio
        high = sink_rate * down_next + ratio * high
        return low, high, up_next, down_next

    up_here = wide_ref[0] + outside
    down_here = wide_ref[levels - 1] + outside
    low = sink_rate * up_here + friction
    high = sink_rate * down_here
    low, high, _, _ = lax.fori_loop(0, levels - 1, eliminate, (low, high, up_here, down_here))

    def keep(k, top, m, bed):
        heavy = top * wide_ref[k]
        for index, step in enumerate((-1, 0, 1)):
            tops[index][k] = moved(top, step, 0)
            heavy_tops[index][k] = moved(heavy, step, 0)
        bed_ref[m + 1] = bed
        heavy_bed[m + 1] = bed * wide_ref[m]

    def substitute(k, carry):
        top, bed = carry
        m = levels - 2 - k
        top = up_ref[m] * top
        bed = bed_ref[k + 2] * bed
        keep(m, top, k + 1, bed)
        return top, bed

    top = inside / low
    bed = inside / (high + friction)
    keep(levels - 1, top, 0, bed)
    zero = jnp.zeros(bed.shape, jnp.float32)
    for ref in (bed_ref, heavy_bed):
        ref[0] = zero
        ref[levels + 1] = zero
    top, bed = lax.fori_loop(0, levels - 1, substitute, (top, bed))
    return top


def couplings(levels, rows, tops, heavy_tops, bed_ref, heavy_bed):
    span_x, span_y = bed_ref.shape[1:]
    offsets = [(dx, dy) for dx in (-1, 0, 1) for dy in (-1, 0, 1) if dx or dy]
    unroll = UNROLL if levels % UNROLL == 0 else 1
    bands = []
    for start in range(0, span_x, rows):
        band = slice(start, start + rows)

        def layer(k, sums):
            reach = {}
            here, sides = bed_ref[k + 1, band], bed_ref[k, band] + bed_ref[k + 2, band]
            v_here = heavy_bed[k + 1, band]
            v_sides = heavy_bed[k, band] + heavy_bed[k + 2, band]
            for count in (1, 2):
                near = offset_weight * 0.5 / count
                far = offset_weight * 0.5 / (count + 1)
                plain, heavy = near * here + far * sides, near * v_here + far * v_sides
                for step_y in (-1, 0, 1):
                    if count == 1 or step_y:
                        reach[count, step_y] = (moved(plain, 0, -step_y), moved(heavy, 0, -step_y))
            out = []
            for (step_x, step_y), total in zip(offsets, sums):
                plain, heavy = reach[abs(step_x) + abs(step_y), step_y]
                top, v_top = tops[step_x + 1][k, band], heavy_tops[step_x + 1][k, band]
                out.append(total + (v_top * plain + top * heavy))
            return tuple(out)

        def layers(block, sums):
            for i in range(unroll):
                sums = layer(block * unroll + i, sums)
            return sums

        zero = jnp.zeros((rows, span_y), jnp.float32)
        bands.append(lax.fori_loop(0, levels // unroll, layers, (zero,) * len(offsets)))
    return {
        (dx, dy): moved(jnp.concatenate([band[i] for band in bands], axis=0), 0, dy)
        for i, (dx, dy) in enumerate(offsets)
    }


def spread(weights, centre, one, two):
    plus = (one + cross_share * two, two + cross_share * one)
    minus = (one - cross_share * two, two - cross_share * one)
    out = [centre * one, centre * two]
    for step_y in (-1, 0, 1):
        side = [moved(x, 0, step_y) for x in (one, two)]
        if step_y:
            pairs = {
                step_y: [moved(x, 0, step_y) for x in plus],
                -step_y: [moved(x, 0, step_y) for x in minus],
            }
            for c in (0, 1):
                out[c] = out[c] + weights[0, step_y] * side[c]
        for step_x in (-1, 1):
            fields = pairs[step_x] if step_y else side
            for c in (0, 1):
                out[c] = out[c] + weights[step_x, step_y] * moved(fields[c], step_x, 0)
    return out


def column_kernel(*refs):
    own_ref, sums_ref, wide_ref = refs[7:10]
    tops, heavy_tops, (bed_ref, heavy_bed) = refs[10:13], refs[13:16], refs[16:18]
    levels, rows, cols = refs[0].shape
    assemble(*refs[0:4], refs[4:7], wide_ref)
    through = vertical(wide_ref, tops, heavy_tops, bed_ref, heavy_bed)
    back = couplings(levels, rows, tops, heavy_tops, bed_ref, heavy_bed)
    forth = {(dx, dy): moved(back[-dx, -dy], dx, dy) for dx, dy in back}
    source = (wide_ref[levels + 1], wide_ref[levels + 2])
    obs, inverse_diag = wide_ref[levels + 3], wide_ref[levels + 4]
    gradient, warm_start = wide_ref[levels + 5], wide_ref[levels + 6]

    def hessian(q):
        surface = spread(forth, through, source[0] * q, source[1] * q)
        basal = spread(back, through, obs * surface[0], obs * surface[1])
        beside = moved(q, 1, 0) + moved(q, -1, 0) + moved(q, 0, 1) + moved(q, 0, -1)
        smooth = reg_gamma * (q + reg_smooth * (4.0 * q - beside))
        return source[0] * basal[0] + source[1] * basal[1] + smooth

    residual = gradient - hessian(warm_start)
    direction = inverse_diag * residual
    image = hessian(direction)
    second = inverse_diag * image
    second_image = hessian(second)
    kept = [x[:rows, :cols] for x in (residual, direction, image, second, second_image)]
    for index, field in enumerate(kept):
        own_ref[index] = field
    residual, direction, image, second, second_image = kept
    parts = (residual * direction, direction * image, second * image, second * second_image)
    rows_of_sums = []
    for part in parts:
        total = jnp.sum(part, axis=0, keepdims=True)
        rows_of_sums.append(sum(total[:, i : i + LANES] for i in range(0, cols, LANES)))
    sums = jnp.concatenate(rows_of_sums, axis=0)
    for device in range(sums_ref.shape[0]):
        sums_ref[device] = sums


def finish_kernel(sums_ref, own_ref, warm_start, solution_ref, residual_ref):
    sums = jnp.sum(jnp.sum(sums_ref[...], axis=0), axis=1, keepdims=True)
    norm_now, curve, cross, second_curve = (sums[i : i + 1] for i in range(4))
    residual, direction, image, second, second_image = (own_ref[i] for i in range(5))
    first_step = norm_now / curve
    norm_next = first_step * first_step * cross - norm_now
    grow = 1.0 + norm_next / norm_now
    next_curve = (
        grow * grow * curve
        - 2.0 * grow * first_step * cross
        + first_step * first_step * second_curve
    )
    next_step = norm_next / next_curve
    solution_ref[...] = (
        warm_start[...]
        + first_step * direction
        + next_step * (grow * direction - first_step * second)
    )
    residual_ref[...] = (
        residual - first_step * image - next_step * (grow * image - first_step * second_image)
    )


def neighbours(axis):
    forward = [(i, i + 1) for i in range(lax.axis_size(axis) - 1)]
    return forward, [(target, source) for source, target in forward]


def on_device(
    gradient, warm_start, viscosity, friction_coef, slide_dir, obs_weight, ice_mask, grounded
):
    levels, rows, cols = viscosity.shape
    sent = jax.ShapeDtypeStruct((-(-(HALO * (levels + FIELDS) + rows) // 8) * 8, cols), jnp.float32)
    packed = jax.ShapeDtypeStruct((rows, -(-(levels + FIELDS) // SLOTS) * LANES), jnp.float32)
    fields, to_low, to_high, first, last = pl.pallas_call(
        field_kernel,
        out_shape=(
            jax.ShapeDtypeStruct((FIELDS, rows, cols), jnp.float32),
            sent,
            sent,
            packed,
            packed,
        ),
        name="fields",
    )(viscosity, gradient, warm_start, friction_coef, slide_dir, obs_weight, ice_mask, grounded)
    next_x, previous_x = neighbours("gx")[::-1]
    next_y, previous_y = neighbours("gy")[::-1]
    row_high = lax.ppermute(to_low, "gx", next_x)
    row_low = lax.ppermute(to_high, "gx", previous_x)
    edges = jnp.stack(
        [lax.ppermute(last, "gy", previous_y), lax.ppermute(first, "gy", next_y)]
    )
    edges = (
        edges,
        lax.ppermute(edges, "gx", next_x),
        lax.ppermute(edges, "gx", previous_x),
    )
    pieces = (viscosity, fields, row_low, row_high)
    devices = lax.axis_size("gx") * lax.axis_size("gy")
    span = (3 * rows, cols + LANES)
    own, sums = pl.pallas_call(
        column_kernel,
        out_shape=(
            jax.ShapeDtypeStruct((5, rows, cols), jnp.float32),
            jax.ShapeDtypeStruct((devices, 4, LANES), jnp.float32),
        ),
        scratch_shapes=[pltpu.VMEM((levels + FIELDS,) + span, jnp.float32)]
        + [pltpu.VMEM((levels,) + span, jnp.float32)] * 6
        + [pltpu.VMEM((levels + 2,) + span, jnp.float32)] * 2,
        name="columns",
    )(*pieces, *edges)
    sums = lax.all_to_all(sums, ("gx", "gy"), 0, 0)
    return pl.pallas_call(
        finish_kernel,
        out_shape=(jax.ShapeDtypeStruct((rows, cols), jnp.float32),) * 2,
        name="finish",
    )(sums, own, warm_start)


def solution(mesh):
    return jax.shard_map(
        on_device,
        mesh=mesh,
        in_specs=(
            P("gx", "gy"),
            P("gx", "gy"),
            P(None, "gx", "gy"),
            P("gx", "gy"),
            P(None, "gx", "gy"),
            P("gx", "gy"),
            P("gx", "gy"),
            P("gx", "gy"),
        ),
        out_specs=(P("gx", "gy"), P("gx", "gy")),
        check_vma=False,
    )
```
